128 devices in a mesh: outer: 8 (over z, y_lo), inner: 4 (over x_lo, core), heads: 4 (over y_hi, x_hi).
Axes of the slice: x: 4 (x_hi: 2, x_lo: 2; x = x_hi * 2 + x_lo), y: 4 (y_hi: 2, y_lo: 2; y = y_hi * 2 + y_lo), z: 4, core: 2. Of those that a mesh axis runs over, the one named last changes fastest.
Arguments:
- raw_keys: bfloat16 [32, 16384, 8, 128], P(None, ('outer', 'inner'), 'heads'), may hold values from -6 to 6
- raw_values: bfloat16 [32, 16384, 8, 128], P(None, ('outer', 'inner'), 'heads'), may hold values from -6 to 6
- turn_angle: float32 [16384, 64], replicated, may hold values from -3.140625 to 3.140625
Outputs:
- stored_keys: bfloat16 [32, 16384, 8, 128], P(('outer', 'inner'), None, 'heads')
- stored_values: bfloat16 [32, 16384, 8, 128], P(('outer', 'inner'), None, 'heads')
- page_high: bfloat16 [32, 256, 8, 128], P(('outer', 'inner'), None, 'heads')
- page_low: bfloat16 [32, 256, 8, 128], P(('outer', 'inner'), None, 'heads')
The draws below stay inside these ranges and needn't reach their ends.
All inputs are finite; a program needn't handle non-finite values.
Results may differ from the reference program's by a relative error of at most 0.001.
Values may be sent and summed in bfloat16 or wider, within the bound.
A program may use at most 128 MiB of HBM per device.

```python
import jax
import jax.numpy as jnp

BATCH = 32
LENGTH = 16384
KV_HEADS = 8
HEAD_SIZE = 128
HALF_HEAD = 64
PAGE = 64


def block_levels(own_key, extent, shards, smallest, largest):
    factor_of = 1.0
    for axis_at, parts in shards:
        steps = jax.random.uniform(jax.random.fold_in(jax.random.fold_in(own_key, 6), axis_at), (parts,), jnp.float32, smallest / len(shards), largest / len(shards))
        factor_of = factor_of * jnp.repeat(jnp.exp(steps), extent[axis_at] // parts).reshape((-1,) + (1,) * (len(extent) - 1 - axis_at))
    return factor_of


def scatter_about(own_key, shape, deviation, most, split=(), dtype=jnp.bfloat16):
    array = deviation * jax.random.normal(own_key, shape, jnp.float32)
    if split:
        array = array * block_levels(own_key, shape, split, -0.22, 0.18)
    return jnp.clip(array, -most, most).astype(dtype)


def setup_inputs(seed: int = 0) -> dict:
    key_list = jax.random.split(jax.random.key(seed), 4)
    raw_keys = scatter_about(key_list[0], (BATCH, LENGTH, KV_HEADS, HEAD_SIZE), 1.0, 6.0, ((1, 32), (2, 4)))
    raw_values = scatter_about(key_list[1], (BATCH, LENGTH, KV_HEADS, HEAD_SIZE), 1.0, 6.0, ((1, 32), (2, 4)))
    turn_angle = jnp.clip(jax.random.uniform(key_list[2], (LENGTH, HALF_HEAD), jnp.float32, -3.140625, 3.140625), -3.140625, 3.140625)
    return {"raw_keys": raw_keys, "raw_values": raw_values, "turn_angle": turn_angle}


def turn_pairs(vectors, angle):
    half = vectors.shape[-1] // 2
    cosine, sine = jnp.cos(angle)[None, :, None, :], jnp.sin(angle)[None, :, None, :]
    first, second = vectors[..., :half], vectors[..., half:]
    return jnp.concatenate([first * cosine - second * sine, second * cosine + first * sine], axis=-1)


def prepare_keys(plain_keys, angle):
    wide_keys = plain_keys.astype(jnp.float32)
    return turn_pairs(wide_keys, angle)


def reference(raw_keys, raw_values, turn_angle):
    turned_keys = prepare_keys(raw_keys, turn_angle)
    narrow_keys = turned_keys.astype(jnp.bfloat16)
    page_view = narrow_keys.reshape(BATCH, LENGTH // PAGE, PAGE, KV_HEADS, HEAD_SIZE)
    page_high = jnp.max(page_view, axis=2)
    page_low = jnp.min(page_view, axis=2)
    stored_keys = narrow_keys
    stored_values = raw_values
    return stored_keys, stored_values, page_high, page_low
```

```python
import jax
import jax.numpy as jnp
from jax import lax
from jax.experimental import pallas as pl
from jax.experimental.pallas import tpu as pltpu
from jax.sharding import PartitionSpec as P

MESH = pl.DeviceIdType.MESH
PAGE = 64
BLOCK = 128

UP, DOWN, BOTH = 1, 3, 2
SLOTS = (
    ((BOTH, 1, 1),),
    ((BOTH, 0, 1), (0, 1, 0)),
    ((BOTH, 1, 0), (0, 0, 1)),
    ((BOTH, 0, 0), (0, 1, 1)),
    ((UP, 1, 1), (DOWN, 0, 0)),
    ((DOWN, 1, 1), (UP, 0, 0)),
    ((UP, 0, 1), (DOWN, 1, 0)),
    ((UP, 1, 0), (DOWN, 0, 1)),
)
ORDER = tuple((*way, core) for slot in SLOTS for core in (0, 1) for way in slot) + ((0, 0, 0, 1),)


def position():
    outer, inner = lax.axis_index("outer"), lax.axis_index("inner")
    return outer // 2, outer % 2, inner // 2, inner % 2


def partner(step):
    z, y, x, core = position()
    return (
        ((z + step[0]) % 4) * 2 + (y + step[1]) % 2,
        ((x + step[2]) % 2) * 2 + (core + step[3]) % 2,
    )


def exchange_kernel(
    keys, values, angle, got_keys, got_values,
    turned, inbox, angles, cosines, sines,
    keys_sent, keys_came, values_sent, values_came, inbox_came, own_came,
):
    parts, rows, size = keys.shape
    heads = 2
    span = rows // heads
    z, y, x, core = position()
    me = (z * 2 + y) * 4 + x * 2 + core

    barrier = pltpu.get_barrier_semaphore()
    for step in ORDER:
        outer, inner = partner(step)
        pl.semaphore_signal(barrier, inc=1, device_id={"outer": outer, "inner": inner}, device_id_type=MESH)
    pl.semaphore_wait(barrier, len(ORDER))

    def send(source, target, sent, came, n):
        outer, inner = partner(ORDER[n])
        return pltpu.make_async_remote_copy(
            src_ref=source.at[outer * 4 + inner],
            dst_ref=target.at[me],
            send_sem=sent.at[n],
            recv_sem=came.at[n],
            device_id={"outer": outer, "inner": inner},
            device_id_type=MESH,
        )

    for n in range(len(ORDER)):
        send(values, got_values, values_sent, values_came, n).start()
    own_values = pltpu.make_async_copy(values.at[me], got_values.at[me], own_came.at[0])
    own_values.start()

    own_angles = pltpu.make_async_copy(
        angle.at[:, pl.ds(pl.multiple_of(me * span, span), span)], angles, own_came.at[1]
    )
    own_angles.start()

    def fetch(i, slot):
        return pltpu.make_async_copy(keys.at[lax.rem(me + 1 + i, parts)], inbox.at[slot], inbox_came.at[slot])

    fetch(0, 0).start()
    own_angles.wait()
    cosine, sine = jnp.cos(angles[...]), jnp.sin(angles[...])
    cosine = jnp.concatenate([cosine, cosine], axis=0).T
    sine = jnp.concatenate([-sine, sine], axis=0).T
    for head in range(heads):
        cosines[pl.ds(head, span, stride=heads), :] = cosine
        sines[pl.ds(head, span, stride=heads), :] = sine

    def turn(slot, target, at):
        def block(b, _):
            here = pl.ds(pl.multiple_of(b * BLOCK, BLOCK), BLOCK)
            wide = inbox[slot, here, :].astype(jnp.float32)
            other = pltpu.roll(wide, size // 2, 1)
            target[at, here, :] = (wide * cosines[here, :] + other * sines[here, :]).astype(jnp.bfloat16)
            return 0

        lax.fori_loop(0, rows // BLOCK, block, 0)

    def chunk(i, _):
        slot = lax.rem(i, 2)
        fetch(i + 1, 1 - slot).start()
        fetch(i, slot).wait()
        turn(slot, turned, lax.rem(me + 1 + i, parts))
        return 0

    lax.fori_loop(0, parts - 1, chunk, 0)
    last = (parts - 1) % 2
    fetch(parts - 1, last).wait()
    turn(last, got_keys, me)

    for n in range(len(ORDER)):
        send(turned, got_keys, keys_sent, keys_came, n).start()
    own_values.wait()
    for n in range(len(ORDER)):
        send(values, got_values, values_sent, values_came, n).wait()
    for n in range(len(ORDER)):
        send(turned, got_keys, keys_sent, keys_came, n).wait()


def store_kernel(got_keys, got_values, keys, values, high, low, highs, lows, flat, stored):
    parts, rows, size = got_keys.shape
    heads = 2
    page = PAGE * heads
    pages = rows // page
    tile = 16
    store_keys = pltpu.make_async_copy(got_keys, keys, stored.at[0])
    store_values = pltpu.make_async_copy(got_values, values, stored.at[1])
    store_keys.start()
    store_values.start()

    def part(s, _):
        for p in range(pages):
            block = [got_keys[s, pl.ds(p * page + t * tile, tile), :] for t in range(page // tile)]
            top, bottom = block[0], block[0]
            for piece in block[1:]:
                top, bottom = jnp.maximum(top, piece), jnp.minimum(bottom, piece)
            here = pl.ds(pl.multiple_of((s * pages + p) * tile, tile), tile)
            highs[here, :] = top.astype(jnp.float32)
            lows[here, :] = bottom.astype(jnp.float32)
        return 0

    lax.fori_loop(0, parts, part, 0)
    count = parts * pages
    for partial, pick, out in ((highs, jnp.maximum, high), (lows, jnp.minimum, low)):
        for head in range(heads):
            best = partial[pl.ds(head, count, stride=tile), :]
            for row in range(heads + head, tile, heads):
                best = pick(best, partial[pl.ds(row, count, stride=tile), :])
            flat[pl.ds(head, count, stride=heads), :] = best
        out[...] = flat[...].astype(jnp.bfloat16)

    store_keys.wait()
    store_values.wait()


def per_device(raw_keys, raw_values, turn_angle):
    parts, span, heads, size = raw_keys.shape
    rows = span * heads
    count = parts * span // PAGE
    steps = len(ORDER)
    near, far = (pl.BlockSpec(memory_space=space) for space in (pltpu.VMEM, pl.ANY))
    cache = (parts, rows, size)
    dma = pltpu.SemaphoreType.DMA
    got_keys, got_values = pl.pallas_call(
        exchange_kernel,
        out_shape=[pltpu.VMEM(cache, jnp.bfloat16)] * 2,
        in_specs=[far] * 3,
        out_specs=[near] * 2,
        scratch_shapes=[
            pltpu.VMEM(cache, jnp.bfloat16),
            pltpu.VMEM((2, rows, size), jnp.bfloat16),
            pltpu.VMEM((turn_angle.shape[1], span), jnp.float32),
            pltpu.VMEM((rows, size), jnp.float32),
            pltpu.VMEM((rows, size), jnp.float32),
            dma((steps,)), dma((steps,)), dma((steps,)), dma((steps,)), dma((2,)), dma((2,)),
        ],
        compiler_params=pltpu.CompilerParams(
            collective_id=0, has_side_effects=True, vmem_limit_bytes=40 * 1024 * 1024
        ),
        name="exchange",
    )(raw_keys.reshape(cache), raw_values.reshape(cache), turn_angle.T)
    keys, values, high, low = pl.pallas_call(
        store_kernel,
        out_shape=[jax.ShapeDtypeStruct(cache, jnp.bfloat16)] * 2
        + [jax.ShapeDtypeStruct((count * heads, size), jnp.bfloat16)] * 2,
        in_specs=[near] * 2,
        out_specs=[far] * 2 + [near] * 2,
        scratch_shapes=[
            pltpu.VMEM((count * 16, size), jnp.float32),
            pltpu.VMEM((count * 16, size), jnp.float32),
            pltpu.VMEM((count * heads, size), jnp.float32),
            dma((2,)),
        ],
        compiler_params=pltpu.CompilerParams(vmem_limit_bytes=24 * 1024 * 1024),
        name="store",
    )(got_keys, got_values)
    whole, bounds = (1, parts * span, heads, size), (1, count, heads, size)
    return keys.reshape(whole), values.reshape(whole), high.reshape(bounds), low.reshape(bounds)


def solution(mesh):
    cut = P(None, ("outer", "inner"), "heads", None)
    kept = P(("outer", "inner"), None, "heads", None)
    return jax.shard_map(
        per_device, mesh=mesh, in_specs=(cut, cut, P()), out_specs=(kept,) * 4, check_vma=False
    )
```

```python
import jax
import jax.numpy as jnp
from jax import lax
from jax.experimental import pallas as pl
from jax.experimental.pallas import tpu as pltpu
from jax.sharding import PartitionSpec as P

MESH = pl.DeviceIdType.MESH
PAGE = 64
BLOCK = 128

UP, DOWN, BOTH = 1, 3, 2
SLOTS = (
    ((BOTH, 1, 1),),
    ((BOTH, 0, 1), (0, 1, 0)),
    ((BOTH, 1, 0), (0, 0, 1)),
    ((BOTH, 0, 0), (0, 1, 1)),
    ((UP, 1, 1), (DOWN, 0, 0)),
    ((DOWN, 1, 1), (UP, 0, 0)),
    ((UP, 0, 1), (DOWN, 1, 0)),
    ((UP, 1, 0), (DOWN, 0, 1)),
)
ORDER = tuple((*way, core) for slot in SLOTS for core in (0, 1) for way in slot) + ((0, 0, 0, 1),)
STARTS = tuple(2 * sum(map(len, SLOTS[:s])) for s in range(len(SLOTS) + 1)) + (len(ORDER),)
GROUPS = tuple(tuple(range(a, b)) for a, b in zip(STARTS, STARTS[1:]))


def position():
    outer, inner = lax.axis_index("outer"), lax.axis_index("inner")
    return outer // 2, outer % 2, inner // 2, inner % 2


def partner(step):
    z, y, x, core = position()
    return (
        ((z + step[0]) % 4) * 2 + (y + step[1]) % 2,
        ((x + step[2]) % 2) * 2 + (core + step[3]) % 2,
    )


def exchange_kernel(
    keys, values, angle, got_keys, got_values,
    turned, angles, cosines, sines,
    keys_sent, keys_came, values_sent, values_came, fetched, own_came,
):
    parts, rows, size = keys.shape
    heads = 2
    span = rows // heads
    z, y, x, core = position()
    me = (z * 2 + y) * 4 + x * 2 + core

    barrier = pltpu.get_barrier_semaphore()
    for step in ORDER:
        outer, inner = partner(step)
        pl.semaphore_signal(barrier, inc=1, device_id={"outer": outer, "inner": inner}, device_id_type=MESH)

    own_angles = pltpu.make_async_copy(
        angle.at[:, pl.ds(pl.multiple_of(me * span, span), span)], angles, own_came.at[0]
    )
    own_keys = pltpu.make_async_copy(keys.at[me], got_keys.at[me], own_came.at[1])
    own_values = pltpu.make_async_copy(values.at[me], got_values.at[me], own_came.at[2])

    def where(n):
        outer, inner = partner(ORDER[n])
        return outer * 4 + inner

    def fetch(n):
        return pltpu.make_async_copy(keys.at[where(n)], turned.at[where(n)], fetched.at[n])

    def send(source, target, sent, came, n):
        outer, inner = partner(ORDER[n])
        return pltpu.make_async_remote_copy(
            src_ref=source.at[outer * 4 + inner],
            dst_ref=target.at[me],
            send_sem=sent.at[n],
            recv_sem=came.at[n],
            device_id={"outer": outer, "inner": inner},
            device_id_type=MESH,
        )

    def send_keys(n):
        return send(turned, got_keys, keys_sent, keys_came, n)

    def send_values(n):
        return send(values, got_values, values_sent, values_came, n)

    pl.semaphore_wait(barrier, len(ORDER))

    for n in GROUPS[0]:
        send_values(n).start()

    own_angles.start()
    for n in range(len(ORDER)):
        fetch(n).start()
    own_keys.start()
    own_values.start()
    own_angles.wait()
    cosine, sine = jnp.cos(angles[...]), jnp.sin(angles[...])
    cosine = jnp.concatenate([cosine, cosine], axis=0).T
    sine = jnp.concatenate([-sine, sine], axis=0).T
    for head in range(heads):
        cosines[pl.ds(head, span, stride=heads), :] = cosine
        sines[pl.ds(head, span, stride=heads), :] = sine

    def turn(cache, at):
        def block(b, _):
            here = pl.ds(pl.multiple_of(b * BLOCK, BLOCK), BLOCK)
            wide = cache[at, here, :].astype(jnp.float32)
            other = pltpu.roll(wide, size // 2, 1)
            cache[at, here, :] = (wide * cosines[here, :] + other * sines[here, :]).astype(jnp.bfloat16)
            return 0

        lax.fori_loop(0, rows // BLOCK, block, 0)

    def turn_group(group):
        for n in group:
            fetch(n).wait()
            turn(turned, where(n))

    for s, group in enumerate(GROUPS):
        if s:
            for n in group:
                send_values(n).start()
        if s == 0:
            turn_group(group)
        if s + 1 < len(GROUPS):
            turn_group(GROUPS[s + 1])
        else:
            own_keys.wait()
            turn(got_keys, me)
        for n in group:
            send_keys(n).start()

    own_values.wait()
    for n in range(len(ORDER)):
        send_values(n).wait()
        send_keys(n).wait()


def store_kernel(got_keys, got_values, keys, values, high, low, highs, lows, flat, bounds, stored):
    parts, rows, size = got_keys.shape
    heads = 2
    page = PAGE * heads
    pages = rows // page
    tile = 16
    store_keys = pltpu.make_async_copy(got_keys, keys, stored.at[0])
    store_values = pltpu.make_async_copy(got_values, values, stored.at[1])
    store_keys.start()
    store_values.start()

    def part(s, _):
        for p in range(pages):
            block = [got_keys[s, pl.ds(p * page + t * tile, tile), :] for t in range(page // tile)]
            top, bottom = block[0], block[0]
            for piece in block[1:]:
                top, bottom = jnp.maximum(top, piece), jnp.minimum(bottom, piece)
            here = pl.ds(pl.multiple_of((s * pages + p) * tile, tile), tile)
            highs[here, :] = top.astype(jnp.float32)
            lows[here, :] = bottom.astype(jnp.float32)
        return 0

    lax.fori_loop(0, parts, part, 0)
    count = parts * pages
    store_bounds = [
        pltpu.make_async_copy(bounds.at[side], out, stored.at[2 + side]) for side, out in enumerate((high, low))
    ]
    for side, (partial, pick) in enumerate(((highs, jnp.maximum), (lows, jnp.minimum))):
        for head in range(heads):
            best = partial[pl.ds(head, count, stride=tile), :]
            for row in range(heads + head, tile, heads):
                best = pick(best, partial[pl.ds(row, count, stride=tile), :])
            flat[pl.ds(head, count, stride=heads), :] = best
        bounds[side] = flat[...].astype(jnp.bfloat16)
    for store in store_bounds:
        store.start()
    for store in (store_keys, store_values, *store_bounds):
        store.wait()


def per_device(raw_keys, raw_values, turn_angle):
    parts, span, heads, size = raw_keys.shape
    rows = span * heads
    count = parts * span // PAGE
    steps = len(ORDER)
    near, far = (pl.BlockSpec(memory_space=space) for space in (pltpu.VMEM, pl.ANY))
    cache = (parts, rows, size)
    dma = pltpu.SemaphoreType.DMA
    got_keys, got_values = pl.pallas_call(
        exchange_kernel,
        out_shape=[pltpu.VMEM(cache, jnp.bfloat16)] * 2,
        in_specs=[far] * 3,
        out_specs=[near] * 2,
        scratch_shapes=[
            pltpu.VMEM(cache, jnp.bfloat16),
            pltpu.VMEM((turn_angle.shape[1], span), jnp.float32),
            pltpu.VMEM((rows, size), jnp.float32),
            pltpu.VMEM((rows, size), jnp.float32),
            dma((steps,)), dma((steps,)), dma((steps,)), dma((steps,)), dma((steps,)), dma((3,)),
        ],
        compiler_params=pltpu.CompilerParams(
            collective_id=0, has_side_effects=True, vmem_limit_bytes=40 * 1024 * 1024
        ),
        name="exchange",
    )(raw_keys.reshape(cache), raw_values.reshape(cache), turn_angle.T)
    keys, values, high, low = pl.pallas_call(
        store_kernel,
        out_shape=[jax.ShapeDtypeStruct(cache, jnp.bfloat16)] * 2
        + [jax.ShapeDtypeStruct((count * heads, size), jnp.bfloat16)] * 2,
        in_specs=[near] * 2,
        out_specs=[far] * 4,
        scratch_shapes=[
            pltpu.VMEM((count * 16, size), jnp.float32),
            pltpu.VMEM((count * 16, size), jnp.float32),
            pltpu.VMEM((count * heads, size), jnp.float32),
            pltpu.VMEM((2, count * heads, size), jnp.bfloat16),
            dma((4,)),
        ],
        compiler_params=pltpu.CompilerParams(vmem_limit_bytes=24 * 1024 * 1024),
        name="store",
    )(got_keys, got_values)
    whole, bounds = (1, parts * span, heads, size), (1, count, heads, size)
    return keys.reshape(whole), values.reshape(whole), high.reshape(bounds), low.reshape(bounds)


def solution(mesh):
    cut = P(None, ("outer", "inner"), "heads", None)
    kept = P(("outer", "inner"), None, "heads", None)
    return jax.shard_map(
        per_device, mesh=mesh, in_specs=(cut, cut, P()), out_specs=(kept,) * 4, check_vma=False
    )
```

```python
import jax
import jax.numpy as jnp
from jax import lax
from jax.experimental import pallas as pl
from jax.experimental.pallas import tpu as pltpu
from jax.sharding import PartitionSpec as P

MESH = pl.DeviceIdType.MESH
PAGE = 64
BLOCK = 256

UP, DOWN, BOTH = 1, 3, 2
SLOTS = (
    ((BOTH, 1, 1),),
    ((BOTH, 0, 1), (0, 1, 0)),
    ((BOTH, 1, 0), (0, 0, 1)),
    ((BOTH, 0, 0), (0, 1, 1)),
    ((UP, 1, 1), (DOWN, 0, 0)),
    ((DOWN, 1, 1), (UP, 0, 0)),
    ((UP, 0, 1), (DOWN, 1, 0)),
    ((UP, 1, 0), (DOWN, 0, 1)),
)
ORDER = tuple((*way, core) for slot in SLOTS for core in (0, 1) for way in slot) + ((0, 0, 0, 1),)
STARTS = tuple(2 * sum(map(len, SLOTS[:s])) for s in range(len(SLOTS) + 1)) + (len(ORDER),)
GROUPS = tuple(tuple(range(a, b)) for a, b in zip(STARTS, STARTS[1:]))


def position():
    outer, inner = lax.axis_index("outer"), lax.axis_index("inner")
    return outer // 2, outer % 2, inner // 2, inner % 2


def partner(step):
    z, y, x, core = position()
    return (
        ((z + step[0]) % 4) * 2 + (y + step[1]) % 2,
        ((x + step[2]) % 2) * 2 + (core + step[3]) % 2,
    )


def exchange_kernel(
    keys, values, angle, got_keys, got_values,
    turned, angles, cosines, sines,
    keys_sent, keys_came, values_sent, values_came, own_came,
):
    parts, rows, size = keys.shape
    heads = 2
    span = rows // heads
    z, y, x, core = position()
    me = (z * 2 + y) * 4 + x * 2 + core

    barrier = pltpu.get_barrier_semaphore()
    for step in ORDER:
        outer, inner = partner(step)
        pl.semaphore_signal(barrier, inc=1, device_id={"outer": outer, "inner": inner}, device_id_type=MESH)

    own_angles = pltpu.make_async_copy(
        angle.at[:, pl.ds(pl.multiple_of(me * span, span), span)], angles, own_came.at[0]
    )
    own_values = pltpu.make_async_copy(values.at[me], got_values.at[me], own_came.at[2])

    all_keys = pltpu.make_async_copy(keys, turned, own_came.at[1])

    def send(source, target, sent, came, n):
        outer, inner = partner(ORDER[n])
        return pltpu.make_async_remote_copy(
            src_ref=source.at[outer * 4 + inner],
            dst_ref=target.at[me],
            send_sem=sent.at[n],
            recv_sem=came.at[n],
            device_id={"outer": outer, "inner": inner},
            device_id_type=MESH,
        )

    def send_keys(n):
        return send(turned, got_keys, keys_sent, keys_came, n)

    def send_values(n):
        return send(values, got_values, values_sent, values_came, n)

    pl.semaphore_wait(barrier, len(ORDER))

    for n in GROUPS[0] + GROUPS[1]:
        send_values(n).start()

    own_angles.start()
    all_keys.start()
    own_values.start()
    own_angles.wait()
    cosine, sine = jnp.cos(angles[...]), jnp.sin(angles[...])
    cosine = jnp.concatenate([cosine, cosine], axis=0).T
    sine = jnp.concatenate([-sine, sine], axis=0).T
    for head in range(heads):
        cosines[pl.ds(head, span, stride=heads), :] = cosine
        sines[pl.ds(head, span, stride=heads), :] = sine

    def turn(source, target, at):
        def block(b, _):
            here = pl.ds(pl.multiple_of(b * BLOCK, BLOCK), BLOCK)
            wide = source[at, here, :].astype(jnp.float32)
            other = pltpu.roll(wide, size // 2, 1)
            target[at, here, :] = (wide * cosines[here, :] + other * sines[here, :]).astype(jnp.bfloat16)
            return 0

        lax.fori_loop(0, rows // BLOCK, block, 0)

    def turn_part(i, _):
        turn(turned, turned, lax.rem(me + 1 + i, parts))
        return 0

    all_keys.wait()
    lax.fori_loop(0, parts - 1, turn_part, 0)
    turn(turned, got_keys, me)
    for n in GROUPS[1] + GROUPS[0]:
        send_keys(n).start()
    for group in GROUPS[2:]:
        for n in group:
            send_values(n).start()
        for n in group:
            send_keys(n).start()

    own_values.wait()
    for n in range(len(ORDER)):
        send_values(n).wait()
        send_keys(n).wait()


def store_kernel(got_keys, got_values, keys, values, high, low, highs, lows, flat, bounds, stored):
    parts, rows, size = got_keys.shape
    heads = 2
    page = PAGE * heads
    pages = rows // page
    tile = 16
    pieces = 8
    stores = [
        pltpu.make_async_copy(got.at[pl.ds(p, parts // pieces)], out.at[pl.ds(p, parts // pieces)], stored.at[side, i])
        for i, p in enumerate(range(0, parts, parts // pieces))
        for side, (got, out) in enumerate(((got_keys, keys), (got_values, values)))
    ]
    for store in stores:
        store.start()

    def part(s, _):
        for p in range(pages):
            block = [got_keys[s, pl.ds(p * page + t * tile, tile), :] for t in range(page // tile)]
            top, bottom = block[0], block[0]
            for piece in block[1:]:
                top, bottom = jnp.maximum(top, piece), jnp.minimum(bottom, piece)
            here = pl.ds(pl.multiple_of((s * pages + p) * tile, tile), tile)
            highs[here, :] = top.astype(jnp.float32)
            lows[here, :] = bottom.astype(jnp.float32)
        return 0

    lax.fori_loop(0, parts, part, 0)
    count = parts * pages
    store_bounds = [
        pltpu.make_async_copy(bounds.at[side], out, stored.at[side, pieces]) for side, out in enumerate((high, low))
    ]
    for side, (partial, pick) in enumerate(((highs, jnp.maximum), (lows, jnp.minimum))):
        for head in range(heads):
            best = partial[pl.ds(head, count, stride=tile), :]
            for row in range(heads + head, tile, heads):
                best = pick(best, partial[pl.ds(row, count, stride=tile), :])
            flat[pl.ds(head, count, stride=heads), :] = best
        bounds[side] = flat[...].astype(jnp.bfloat16)
    for store in store_bounds:
        store.start()
    for store in (*stores, *store_bounds):
        store.wait()


def per_device(raw_keys, raw_values, turn_angle):
    parts, span, heads, size = raw_keys.shape
    rows = span * heads
    count = parts * span // PAGE
    steps = len(ORDER)
    near, far = (pl.BlockSpec(memory_space=space) for space in (pltpu.VMEM, pl.ANY))
    cache = (parts, rows, size)
    dma = pltpu.SemaphoreType.DMA
    got_keys, got_values = pl.pallas_call(
        exchange_kernel,
        out_shape=[pltpu.VMEM(cache, jnp.bfloat16)] * 2,
        in_specs=[far] * 3,
        out_specs=[near] * 2,
        scratch_shapes=[
            pltpu.VMEM(cache, jnp.bfloat16),
            pltpu.VMEM((turn_angle.shape[1], span), jnp.float32),
            pltpu.VMEM((rows, size), jnp.float32),
            pltpu.VMEM((rows, size), jnp.float32),
            dma((steps,)), dma((steps,)), dma((steps,)), dma((steps,)), dma((3,)),
        ],
        compiler_params=pltpu.CompilerParams(
            collective_id=0, has_side_effects=True, vmem_limit_bytes=40 * 1024 * 1024
        ),
        name="exchange",
    )(raw_keys.reshape(cache), raw_values.reshape(cache), turn_angle.T)
    keys, values, high, low = pl.pallas_call(
        store_kernel,
        out_shape=[jax.ShapeDtypeStruct(cache, jnp.bfloat16)] * 2
        + [jax.ShapeDtypeStruct((count * heads, size), jnp.bfloat16)] * 2,
        in_specs=[near] * 2,
        out_specs=[far] * 4,
        scratch_shapes=[
            pltpu.VMEM((count * 16, size), jnp.float32),
            pltpu.VMEM((count * 16, size), jnp.float32),
            pltpu.VMEM((count * heads, size), jnp.float32),
            pltpu.VMEM((2, count * heads, size), jnp.bfloat16),
            dma((2, 9)),
        ],
        compiler_params=pltpu.CompilerParams(vmem_limit_bytes=24 * 1024 * 1024),
        name="store",
    )(got_keys, got_values)
    whole, bounds = (1, parts * span, heads, size), (1, count, heads, size)
    return keys.reshape(whole), values.reshape(whole), high.reshape(bounds), low.reshape(bounds)


def solution(mesh):
    cut = P(None, ("outer", "inner"), "heads", None)
    kept = P(("outer", "inner"), None, "heads", None)
    return jax.shard_map(
        per_device, mesh=mesh, in_specs=(cut, cut, P()), out_specs=(kept,) * 4, check_vma=False
    )
```

```python
import jax
import jax.numpy as jnp
from jax import lax
from jax.experimental import pallas as pl
from jax.experimental.pallas import tpu as pltpu
from jax.sharding import PartitionSpec as P

MESH = pl.DeviceIdType.MESH
PAGE = 64
BLOCK = 256

UP, DOWN, BOTH = 1, 3, 2
SLOTS = (
    ((BOTH, 1, 1),),
    ((BOTH, 0, 1), (0, 1, 0)),
    ((BOTH, 1, 0), (0, 0, 1)),
    ((BOTH, 0, 0), (0, 1, 1)),
    ((UP, 1, 1), (DOWN, 0, 0)),
    ((DOWN, 1, 1), (UP, 0, 0)),
    ((UP, 0, 1), (DOWN, 1, 0)),
    ((UP, 1, 0), (DOWN, 0, 1)),
)
ORDER = tuple((*way, core) for slot in SLOTS for core in (0, 1) for way in slot) + ((0, 0, 0, 1),)
STARTS = tuple(2 * sum(map(len, SLOTS[:s])) for s in range(len(SLOTS) + 1)) + (len(ORDER),)
GROUPS = tuple(tuple(range(a, b)) for a, b in zip(STARTS, STARTS[1:]))


def position():
    outer, inner = lax.axis_index("outer"), lax.axis_index("inner")
    return outer // 2, outer % 2, inner // 2, inner % 2


def partner(step):
    z, y, x, core = position()
    return (
        ((z + step[0]) % 4) * 2 + (y + step[1]) % 2,
        ((x + step[2]) % 2) * 2 + (core + step[3]) % 2,
    )


def exchange_kernel(
    keys, values, angle, got_keys, got_values,
    turned, first, angles, cosines, sines,
    keys_sent, keys_came, values_sent, values_came, first_came, own_came,
):
    parts, rows, size = keys.shape
    heads = 2
    span = rows // heads
    z, y, x, core = position()
    me = (z * 2 + y) * 4 + x * 2 + core

    def fetch_first(n):
        outer, inner = partner(ORDER[n])
        return pltpu.make_async_copy(values.at[outer * 4 + inner], first.at[n], first_came.at[n])

    for n in GROUPS[0]:
        fetch_first(n).start()

    barrier = pltpu.get_barrier_semaphore()
    for step in ORDER:
        outer, inner = partner(step)
        pl.semaphore_signal(barrier, inc=1, device_id={"outer": outer, "inner": inner}, device_id_type=MESH)

    own_angles = pltpu.make_async_copy(
        angle.at[:, pl.ds(pl.multiple_of(me * span, span), span)], angles, own_came.at[0]
    )
    own_values = pltpu.make_async_copy(values.at[me], got_values.at[me], own_came.at[2])

    all_keys = pltpu.make_async_copy(keys, turned, own_came.at[1])

    def send(source, target, sent, came, n, held=None):
        outer, inner = partner(ORDER[n])
        return pltpu.make_async_remote_copy(
            src_ref=source.at[outer * 4 + inner] if held is None else held,
            dst_ref=target.at[me],
            send_sem=sent.at[n],
            recv_sem=came.at[n],
            device_id={"outer": outer, "inner": inner},
            device_id_type=MESH,
        )

    def send_keys(n):
        return send(turned, got_keys, keys_sent, keys_came, n)

    def send_values(n):
        return send(values, got_values, values_sent, values_came, n, first.at[n] if n in GROUPS[0] else None)

    pl.semaphore_wait(barrier, len(ORDER))

    for n in GROUPS[0]:
        fetch_first(n).wait()
    for n in GROUPS[0] + GROUPS[1]:
        send_values(n).start()

    own_angles.start()
    all_keys.start()
    own_values.start()
    own_angles.wait()
    cosine, sine = jnp.cos(angles[...]), jnp.sin(angles[...])
    cosine = jnp.concatenate([cosine, cosine], axis=0).T
    sine = jnp.concatenate([-sine, sine], axis=0).T
    for head in range(heads):
        cosines[pl.ds(head, span, stride=heads), :] = cosine
        sines[pl.ds(head, span, stride=heads), :] = sine

    def turn(source, target, at):
        def block(b, _):
            here = pl.ds(pl.multiple_of(b * BLOCK, BLOCK), BLOCK)
            wide = source[at, here, :].astype(jnp.float32)
            other = pltpu.roll(wide, size // 2, 1)
            target[at, here, :] = (wide * cosines[here, :] + other * sines[here, :]).astype(jnp.bfloat16)
            return 0

        lax.fori_loop(0, rows // BLOCK, block, 0)

    def turn_part(i, _):
        turn(turned, turned, lax.rem(me + 1 + i, parts))
        return 0

    all_keys.wait()
    lax.fori_loop(0, parts - 1, turn_part, 0)
    turn(turned, got_keys, me)
    for n in GROUPS[1] + GROUPS[0]:
        send_keys(n).start()
    for group in GROUPS[2:]:
        for n in group:
            send_values(n).start()
        for n in group:
            send_keys(n).start()

    own_values.wait()
    for n in range(len(ORDER)):
        send_values(n).wait()
        send_keys(n).wait()


def store_kernel(got_keys, got_values, keys, values, high, low, highs, lows, flat, bounds, stored):
    parts, rows, size = got_keys.shape
    heads = 2
    page = PAGE * heads
    pages = rows // page
    tile = 16
    pieces = 8
    stores = [
        pltpu.make_async_copy(got.at[pl.ds(p, parts // pieces)], out.at[pl.ds(p, parts // pieces)], stored.at[side, i])
        for i, p in enumerate(range(0, parts, parts // pieces))
        for side, (got, out) in enumerate(((got_keys, keys), (got_values, values)))
    ]
    for store in stores:
        store.start()

    def part(s, _):
        for p in range(pages):
            block = [got_keys[s, pl.ds(p * page + t * tile, tile), :] for t in range(page // tile)]
            top, bottom = block[0], block[0]
            for piece in block[1:]:
                top, bottom = jnp.maximum(top, piece), jnp.minimum(bottom, piece)
            here = pl.ds(pl.multiple_of((s * pages + p) * tile, tile), tile)
            highs[here, :] = top.astype(jnp.float32)
            lows[here, :] = bottom.astype(jnp.float32)
        return 0

    lax.fori_loop(0, parts, part, 0)
    count = parts * pages
    store_bounds = [
        pltpu.make_async_copy(bounds.at[side], out, stored.at[side, pieces]) for side, out in enumerate((high, low))
    ]
    for side, (partial, pick) in enumerate(((highs, jnp.maximum), (lows, jnp.minimum))):
        for head in range(heads):
            best = partial[pl.ds(head, count, stride=tile), :]
            for row in range(heads + head, tile, heads):
                best = pick(best, partial[pl.ds(row, count, stride=tile), :])
            flat[pl.ds(head, count, stride=heads), :] = best
        bounds[side] = flat[...].astype(jnp.bfloat16)
    for store in store_bounds:
        store.start()
    for store in (*stores, *store_bounds):
        store.wait()


def per_device(raw_keys, raw_values, turn_angle):
    parts, span, heads, size = raw_keys.shape
    rows = span * heads
    count = parts * span // PAGE
    steps = len(ORDER)
    near, far = (pl.BlockSpec(memory_space=space) for space in (pltpu.VMEM, pl.ANY))
    cache = (parts, rows, size)
    dma = pltpu.SemaphoreType.DMA
    got_keys, got_values = pl.pallas_call(
        exchange_kernel,
        out_shape=[pltpu.VMEM(cache, jnp.bfloat16)] * 2,
        in_specs=[far] * 3,
        out_specs=[near] * 2,
        scratch_shapes=[
            pltpu.VMEM(cache, jnp.bfloat16),
            pltpu.VMEM((len(GROUPS[0]), rows, size), jnp.bfloat16),
            pltpu.VMEM((turn_angle.shape[1], span), jnp.float32),
            pltpu.VMEM((rows, size), jnp.float32),
            pltpu.VMEM((rows, size), jnp.float32),
            dma((steps,)), dma((steps,)), dma((steps,)), dma((steps,)), dma((len(GROUPS[0]),)), dma((3,)),
        ],
        compiler_params=pltpu.CompilerParams(
            collective_id=0, has_side_effects=True, vmem_limit_bytes=40 * 1024 * 1024
        ),
        name="exchange",
    )(raw_keys.reshape(cache), raw_values.reshape(cache), turn_angle.T)
    keys, values, high, low = pl.pallas_call(
        store_kernel,
        out_shape=[jax.ShapeDtypeStruct(cache, jnp.bfloat16)] * 2
        + [jax.ShapeDtypeStruct((count * heads, size), jnp.bfloat16)] * 2,
        in_specs=[near] * 2,
        out_specs=[far] * 4,
        scratch_shapes=[
            pltpu.VMEM((count * 16, size), jnp.float32),
            pltpu.VMEM((count * 16, size), jnp.float32),
            pltpu.VMEM((count * heads, size), jnp.float32),
            pltpu.VMEM((2, count * heads, size), jnp.bfloat16),
            dma((2, 9)),
        ],
        compiler_params=pltpu.CompilerParams(vmem_limit_bytes=24 * 1024 * 1024),
        name="store",
    )(got_keys, got_values)
    whole, bounds = (1, parts * span, heads, size), (1, count, heads, size)
    return keys.reshape(whole), values.reshape(whole), high.reshape(bounds), low.reshape(bounds)


def solution(mesh):
    cut = P(None, ("outer", "inner"), "heads", None)
    kept = P(("outer", "inner"), None, "heads", None)
    return jax.shard_map(
        per_device, mesh=mesh, in_specs=(cut, cut, P()), out_specs=(kept,) * 4, check_vma=False
    )
```

```python
import jax
import jax.numpy as jnp
from jax import lax
from jax.experimental import pallas as pl
from jax.experimental.pallas import tpu as pltpu
from jax.sharding import PartitionSpec as P

MESH = pl.DeviceIdType.MESH
PAGE = 64
BLOCK = 256

UP, DOWN, BOTH = 1, 3, 2
SLOTS = (
    ((BOTH, 1, 1),),
    ((BOTH, 0, 1), (0, 1, 0)),
    ((BOTH, 1, 0), (0, 0, 1)),
    ((BOTH, 0, 0), (0, 1, 1)),
    ((UP, 1, 1), (DOWN, 0, 0)),
    ((DOWN, 1, 1), (UP, 0, 0)),
    ((UP, 0, 1), (DOWN, 1, 0)),
    ((UP, 1, 0), (DOWN, 0, 1)),
)
ORDER = tuple((*way, core) for slot in SLOTS for core in (0, 1) for way in slot) + ((0, 0, 0, 1),)
STARTS = tuple(2 * sum(map(len, SLOTS[:s])) for s in range(len(SLOTS) + 1)) + (len(ORDER),)
GROUPS = tuple(tuple(range(a, b)) for a, b in zip(STARTS, STARTS[1:]))


def position():
    outer, inner = lax.axis_index("outer"), lax.axis_index("inner")
    z, x = lax.div(outer, 2), lax.div(inner, 2)
    return z, outer - 2 * z, x, inner - 2 * x


def partner(step):
    z, y, x, core = position()
    flip = lambda bit, over: 1 - bit if over else bit
    return lax.rem(z + step[0], 4) * 2 + flip(y, step[1]), flip(x, step[2]) * 2 + flip(core, step[3])


def exchange_kernel(
    keys, values, angle, got_keys, got_values,
    turned, first, angles, cosines, sines,
    keys_sent, keys_came, values_sent, values_came, first_came, own_came,
):
    parts, rows, size = keys.shape
    heads = 2
    span = rows // heads
    z, y, x, core = position()
    me = (z * 2 + y) * 4 + x * 2 + core

    def fetch_first(n):
        outer, inner = partner(ORDER[n])
        return pltpu.make_async_copy(values.at[outer * 4 + inner], first.at[n], first_came.at[n])

    for n in GROUPS[0]:
        fetch_first(n).start()

    barrier = pltpu.get_barrier_semaphore()
    for step in ORDER:
        outer, inner = partner(step)
        pl.semaphore_signal(barrier, inc=1, device_id={"outer": outer, "inner": inner}, device_id_type=MESH)

    own_angles = pltpu.make_async_copy(
        angle.at[:, pl.ds(pl.multiple_of(me * span, span), span)], angles, own_came.at[0]
    )
    own_values = pltpu.make_async_copy(values.at[me], got_values.at[me], own_came.at[2])

    all_keys = pltpu.make_async_copy(keys, turned, own_came.at[1])

    def send(source, target, sent, came, n, held=None):
        outer, inner = partner(ORDER[n])
        return pltpu.make_async_remote_copy(
            src_ref=source.at[outer * 4 + inner] if held is None else held,
            dst_ref=target.at[me],
            send_sem=sent.at[n],
            recv_sem=came.at[n],
            device_id={"outer": outer, "inner": inner},
            device_id_type=MESH,
        )

    def send_keys(n):
        return send(turned, got_keys, keys_sent, keys_came, n)

    def send_values(n):
        return send(values, got_values, values_sent, values_came, n, first.at[n] if n in GROUPS[0] else None)

    pl.semaphore_wait(barrier, len(ORDER))

    for n in GROUPS[0]:
        fetch_first(n).wait()
    for n in GROUPS[0] + GROUPS[1]:
        send_values(n).start()

    own_angles.start()
    all_keys.start()
    own_values.start()
    own_angles.wait()
    cosine, sine = jnp.cos(angles[...]), jnp.sin(angles[...])
    cosine = jnp.concatenate([cosine, cosine], axis=0).T
    sine = jnp.concatenate([-sine, sine], axis=0).T
    for head in range(heads):
        cosines[pl.ds(head, span, stride=heads), :] = cosine
        sines[pl.ds(head, span, stride=heads), :] = sine

    def turn(source, target, at):
        def block(b, _):
            here = pl.ds(pl.multiple_of(b * BLOCK, BLOCK), BLOCK)
            wide = source[at, here, :].astype(jnp.float32)
            other = pltpu.roll(wide, size // 2, 1)
            target[at, here, :] = (wide * cosines[here, :] + other * sines[here, :]).astype(jnp.bfloat16)
            return 0

        lax.fori_loop(0, rows // BLOCK, block, 0)

    def turn_part(i, _):
        turn(turned, turned, lax.rem(me + 1 + i, parts))
        return 0

    all_keys.wait()
    lax.fori_loop(0, parts - 1, turn_part, 0)
    turn(turned, got_keys, me)
    for n in GROUPS[1] + GROUPS[0]:
        send_keys(n).start()
    for group in GROUPS[2:]:
        for n in group:
            send_values(n).start()
        for n in group:
            send_keys(n).start()

    own_values.wait()
    for n in range(len(ORDER)):
        send_values(n).wait()
        send_keys(n).wait()


def store_kernel(got_keys, got_values, keys, values, high, low, highs, lows, flat, bounds, stored):
    parts, rows, size = got_keys.shape
    heads = 2
    page = PAGE * heads
    pages = rows // page
    tile = 16
    pieces = 8
    stores = [
        pltpu.make_async_copy(got.at[pl.ds(p, parts // pieces)], out.at[pl.ds(p, parts // pieces)], stored.at[side, i])
        for i, p in enumerate(range(0, parts, parts // pieces))
        for side, (got, out) in enumerate(((got_keys, keys), (got_values, values)))
    ]
    for store in stores:
        store.start()

    def part(s, _):
        for p in range(pages):
            block = [got_keys[s, pl.ds(p * page + t * tile, tile), :] for t in range(page // tile)]
            top, bottom = block[0], block[0]
            for piece in block[1:]:
                top, bottom = jnp.maximum(top, piece), jnp.minimum(bottom, piece)
            here = pl.ds(pl.multiple_of((s * pages + p) * tile, tile), tile)
            highs[here, :] = top.astype(jnp.float32)
            lows[here, :] = bottom.astype(jnp.float32)
        return 0

    lax.fori_loop(0, parts, part, 0)
    count = parts * pages
    store_bounds = [
        pltpu.make_async_copy(bounds.at[side], out, stored.at[side, pieces]) for side, out in enumerate((high, low))
    ]
    for side, (partial, pick) in enumerate(((highs, jnp.maximum), (lows, jnp.minimum))):
        for head in range(heads):
            best = partial[pl.ds(head, count, stride=tile), :]
            for row in range(heads + head, tile, heads):
                best = pick(best, partial[pl.ds(row, count, stride=tile), :])
            flat[pl.ds(head, count, stride=heads), :] = best
        bounds[side] = flat[...].astype(jnp.bfloat16)
    for store in store_bounds:
        store.start()
    for store in (*stores, *store_bounds):
        store.wait()


def per_device(raw_keys, raw_values, turn_angle):
    parts, span, heads, size = raw_keys.shape
    rows = span * heads
    count = parts * span // PAGE
    steps = len(ORDER)
    near, far = (pl.BlockSpec(memory_space=space) for space in (pltpu.VMEM, pl.ANY))
    cache = (parts, rows, size)
    dma = pltpu.SemaphoreType.DMA
    got_keys, got_values = pl.pallas_call(
        exchange_kernel,
        out_shape=[pltpu.VMEM(cache, jnp.bfloat16)] * 2,
        in_specs=[far] * 3,
        out_specs=[near] * 2,
        scratch_shapes=[
            pltpu.VMEM(cache, jnp.bfloat16),
            pltpu.VMEM((len(GROUPS[0]), rows, size), jnp.bfloat16),
            pltpu.VMEM((turn_angle.shape[1], span), jnp.float32),
            pltpu.VMEM((rows, size), jnp.float32),
            pltpu.VMEM((rows, size), jnp.float32),
            dma((steps,)), dma((steps,)), dma((steps,)), dma((steps,)), dma((len(GROUPS[0]),)), dma((3,)),
        ],
        compiler_params=pltpu.CompilerParams(
            collective_id=0, has_side_effects=True, vmem_limit_bytes=40 * 1024 * 1024
        ),
        name="exchange",
    )(raw_keys.reshape(cache), raw_values.reshape(cache), turn_angle.T)
    keys, values, high, low = pl.pallas_call(
        store_kernel,
        out_shape=[jax.ShapeDtypeStruct(cache, jnp.bfloat16)] * 2
        + [jax.ShapeDtypeStruct((count * heads, size), jnp.bfloat16)] * 2,
        in_specs=[near] * 2,
        out_specs=[far] * 4,
        scratch_shapes=[
            pltpu.VMEM((count * 16, size), jnp.float32),
            pltpu.VMEM((count * 16, size), jnp.float32),
            pltpu.VMEM((count * heads, size), jnp.float32),
            pltpu.VMEM((2, count * heads, size), jnp.bfloat16),
            dma((2, 9)),
        ],
        compiler_params=pltpu.CompilerParams(vmem_limit_bytes=24 * 1024 * 1024),
        name="store",
    )(got_keys, got_values)
    whole, bounds = (1, parts * span, heads, size), (1, count, heads, size)
    return keys.reshape(whole), values.reshape(whole), high.reshape(bounds), low.reshape(bounds)


def solution(mesh):
    cut = P(None, ("outer", "inner"), "heads", None)
    kept = P(("outer", "inner"), None, "heads", None)
    return jax.shard_map(
        per_device, mesh=mesh, in_specs=(cut, cut, P()), out_specs=(kept,) * 4, check_vma=False
    )
```
